128 devices in a mesh: dp: 1, cpo: 2 (over core), cpi: 64 (over z, y, x).
Axes of the slice: x: 4, y: 4, z: 4, core: 2. Of those that a mesh axis runs over, the one named last changes fastest.
Arguments:
- hidden: bfloat16 [32768, 4608], P(('dp', 'cpo', 'cpi'))
- w_q: bfloat16 [4608, 32, 128], replicated
- w_k: bfloat16 [4608, 16, 128], replicated
- w_v: bfloat16 [4608, 16, 128], replicated
- w_o: bfloat16 [32, 128, 4608], replicated
Outputs:
- output: bfloat16 [32768, 4608], P(('dp', 'cpo', 'cpi'))
All inputs are finite; a program needn't handle non-finite values.
Results may differ from the reference program's by a relative error of at most 0.00592278.
Values are sent between devices in bfloat16 or wider.
A program may use at most 1 GiB of HBM per device.

```python
import jax
import jax.numpy as jnp
from jax import lax

D_MODEL = 4608
HEADS_Q = 32
HEADS_KV = 16
HEAD_DIM = 128
TOK_DEV = 256
CHUNKS = 128
WINDOW = 2048
QUERY_BLOCK = 128
SEQ_LEN = CHUNKS * TOK_DEV
GROUP_SIZE = HEADS_Q // HEADS_KV
KEY_SPAN = WINDOW + QUERY_BLOCK
ROPE_BASE = 10000.0


def setup_inputs(seed: int = 0, part: int = 0) -> dict:
    root_part, root_shared = jax.random.split(jax.random.key(seed))
    key_noise, key_shift = jax.random.split(jax.random.fold_in(root_part, part))
    key_q, key_k, key_v, key_o = jax.random.split(root_shared, 4)
    noise = jax.random.normal(key_noise, (CHUNKS, TOK_DEV, D_MODEL), jnp.float32)
    shifts = jax.random.normal(key_shift, (CHUNKS, 1, D_MODEL), jnp.float32)
    hidden = (0.8 * noise + 0.8 * shifts).reshape(SEQ_LEN, D_MODEL).astype(jnp.bfloat16)
    scale_in = D_MODEL ** -0.5
    scale_out = (HEADS_Q * HEAD_DIM) ** -0.5
    w_q = (jax.random.normal(key_q, (D_MODEL, HEADS_Q, HEAD_DIM), jnp.float32) * scale_in).astype(jnp.bfloat16)
    w_k = (jax.random.normal(key_k, (D_MODEL, HEADS_KV, HEAD_DIM), jnp.float32) * scale_in).astype(jnp.bfloat16)
    w_v = (jax.random.normal(key_v, (D_MODEL, HEADS_KV, HEAD_DIM), jnp.float32) * scale_in).astype(jnp.bfloat16)
    w_o = (jax.random.normal(key_o, (HEADS_Q, HEAD_DIM, D_MODEL), jnp.float32) * scale_out).astype(jnp.bfloat16)
    return {'hidden': hidden, 'w_q': w_q, 'w_k': w_k, 'w_v': w_v, 'w_o': w_o}


def rope_rotate(vals, positions):
    half_dim = HEAD_DIM // 2
    inv_freq = ROPE_BASE ** (-jnp.arange(half_dim, dtype=jnp.float32) * 2.0 / HEAD_DIM)
    angles = positions.astype(jnp.float32)[..., None] * inv_freq
    cos_t = jnp.cos(angles)[..., None, :]
    sin_t = jnp.sin(angles)[..., None, :]
    lower_half = vals[..., :half_dim]
    upper_half = vals[..., half_dim:]
    return jnp.concatenate([lower_half * cos_t - upper_half * sin_t, upper_half * cos_t + lower_half * sin_t], axis=-1)


def reference(hidden, w_q, w_k, w_v, w_o):
    positions = jnp.arange(SEQ_LEN)
    q_proj = jnp.dot(hidden, w_q.reshape(D_MODEL, HEADS_Q * HEAD_DIM), preferred_element_type=jnp.float32)
    k_proj = jnp.dot(hidden, w_k.reshape(D_MODEL, HEADS_KV * HEAD_DIM), preferred_element_type=jnp.float32)
    v_proj = jnp.dot(hidden, w_v.reshape(D_MODEL, HEADS_KV * HEAD_DIM), preferred_element_type=jnp.float32)
    q_rot = rope_rotate(q_proj.reshape(SEQ_LEN, HEADS_Q, HEAD_DIM), positions).astype(jnp.bfloat16)
    k_rot = rope_rotate(k_proj.reshape(SEQ_LEN, HEADS_KV, HEAD_DIM), positions).astype(jnp.bfloat16)
    v_val = v_proj.reshape(SEQ_LEN, HEADS_KV, HEAD_DIM).astype(jnp.bfloat16)
    k_pad = jnp.concatenate([jnp.zeros((WINDOW, HEADS_KV, HEAD_DIM), jnp.bfloat16), k_rot], axis=0)
    v_pad = jnp.concatenate([jnp.zeros((WINDOW, HEADS_KV, HEAD_DIM), jnp.bfloat16), v_val], axis=0)
    score_scale = HEAD_DIM ** -0.5
    q_offsets = jnp.arange(QUERY_BLOCK)
    k_offsets = jnp.arange(KEY_SPAN)

    def attend_block(block_idx):
        q_start = block_idx * QUERY_BLOCK
        q_blk = lax.dynamic_slice_in_dim(q_rot, q_start, QUERY_BLOCK, 0).reshape(QUERY_BLOCK, HEADS_KV, GROUP_SIZE, HEAD_DIM)
        k_blk = lax.dynamic_slice_in_dim(k_pad, q_start, KEY_SPAN, 0)
        v_blk = lax.dynamic_slice_in_dim(v_pad, q_start, KEY_SPAN, 0)
        scores = jnp.einsum('tkgd,skd->kgts', q_blk.astype(jnp.float32), k_blk.astype(jnp.float32)) * score_scale
        pos_gap = q_offsets[:, None] + WINDOW - k_offsets[None, :]
        key_pos = q_start - WINDOW + k_offsets
        allowed = (pos_gap >= 0) & (pos_gap < WINDOW) & (key_pos[None, :] >= 0)
        scores = jnp.where(allowed, scores, -jnp.inf)
        row_max = jnp.max(scores, axis=-1, keepdims=True)
        exp_scores = jnp.exp(scores - row_max)
        exp_total = jnp.sum(exp_scores, axis=-1)
        weighted = jnp.einsum('kgts,skd->kgtd', exp_scores.astype(jnp.bfloat16).astype(jnp.float32), v_blk.astype(jnp.float32))
        return (weighted / exp_total[..., None]).astype(jnp.bfloat16)

    attended = lax.map(attend_block, jnp.arange(SEQ_LEN // QUERY_BLOCK))
    attended = jnp.transpose(attended, (0, 3, 1, 2, 4)).reshape(SEQ_LEN, HEADS_Q * HEAD_DIM)
    out_proj = jnp.dot(attended, w_o.reshape(HEADS_Q * HEAD_DIM, D_MODEL), preferred_element_type=jnp.float32)
    return out_proj.astype(jnp.bfloat16)
```

```python
import functools
import math

import jax
import jax.numpy as jnp
from jax import lax
from jax.experimental import pallas as pl
from jax.experimental.pallas import tpu as pltpu
from jax.sharding import PartitionSpec as P

ROPE_BASE = 10000.0
GROUP = 16
TOK = 256
HD = 128
BACK = 8
MESH = pl.DeviceIdType.MESH


def head_of(member):
    y = member // 4
    x = member % 4
    d = (x + 4 - y) % 4
    return 8 * (d % 2) + 4 * (d // 2) + y


def member_of(head):
    c = head // 8
    b = (head // 4) % 2
    y = head % 4
    return 4 * y + (y + c + 2 * b) % 4


def body(x_hbm, wq_hbm, wk_hbm, wv_hbm, wo_hbm, cos_hbm, sin_hbm, y_hbm,
         x_v, cos_v, sin_v, w0, w1, kv_out, q_out, kv_in, q_in, s_buf, o_out, o_in, wo_buf, y_acc, y_bf,
         in_sem, w_sem, wo_sem, y_sem, kv_ss, kv_rs, h_ss, h_rs, q_ss, q_rs, o_ss, o_rs):
    core = lax.axis_index('cpo')
    chip = lax.axis_index('cpi')
    z = chip // GROUP
    me = chip % GROUP
    base = z * GROUP
    my_head = head_of(me)
    d_model = x_v.shape[1]

    wk_first = pltpu.make_async_copy(wk_hbm.at[:, pl.ds(0, 8), :], w0, w_sem.at[0])
    wv_first = pltpu.make_async_copy(wv_hbm.at[:, pl.ds(0, 8), :], w1, w_sem.at[1])
    x_copy = pltpu.make_async_copy(x_hbm, x_v, in_sem.at[0])
    cos_copy = pltpu.make_async_copy(cos_hbm, cos_v, in_sem.at[1])
    sin_copy = pltpu.make_async_copy(sin_hbm, sin_v, in_sem.at[2])
    x_copy.start()
    cos_copy.start()
    sin_copy.start()
    wk_first.start()
    wv_first.start()

    next_core = jnp.where(z == 3, 1 - core, core)
    next_chip = ((z + 1) % 4) * GROUP + me
    prev_core = jnp.where(z == 0, 1 - core, core)
    prev_chip = ((z + 3) % 4) * GROUP + me

    barrier = pltpu.get_barrier_semaphore()
    for step in range(1, GROUP):
        pl.semaphore_signal(barrier, inc=1, device_id={'cpi': base + (me + step) % GROUP}, device_id_type=MESH)
    pl.semaphore_signal(barrier, inc=1, device_id={'cpo': next_core, 'cpi': next_chip}, device_id_type=MESH)
    pl.semaphore_signal(barrier, inc=1, device_id={'cpo': prev_core, 'cpi': prev_chip}, device_id_type=MESH)
    pl.semaphore_wait(barrier, GROUP + 1)

    x_copy.wait()
    cos_copy.wait()
    sin_copy.wait()

    def project(w_ref):
        w = w_ref[...].reshape(d_model, 8 * HD)
        return jnp.dot(x_v[...], w, preferred_element_type=jnp.float32)

    def rope(u):
        return u * cos_v[...] + pltpu.roll(u, HD // 2, 1) * sin_v[...]

    def kv_send(head):
        return pltpu.make_async_remote_copy(
            src_ref=kv_out.at[head], dst_ref=kv_in.at[BACK + me], send_sem=kv_ss.at[head], recv_sem=kv_rs.at[me],
            device_id={'cpi': base + member_of(head)}, device_id_type=MESH)

    def q_send(head):
        return pltpu.make_async_remote_copy(
            src_ref=q_out.at[head], dst_ref=q_in.at[me], send_sem=q_ss.at[head], recv_sem=q_rs.at[me],
            device_id={'cpi': base + member_of(head)}, device_id_type=MESH)

    def kv_recv(src):
        return pltpu.make_async_remote_copy(
            src_ref=kv_in.at[BACK + src], dst_ref=kv_in.at[BACK + src], send_sem=kv_ss.at[0], recv_sem=kv_rs.at[src],
            device_id={'cpi': base + src}, device_id_type=MESH)

    def q_recv(src):
        return pltpu.make_async_remote_copy(
            src_ref=q_in.at[src], dst_ref=q_in.at[src], send_sem=q_ss.at[0], recv_sem=q_rs.at[src],
            device_id={'cpi': base + src}, device_id_type=MESH)

    def halo(block):
        return pltpu.make_async_remote_copy(
            src_ref=kv_in.at[GROUP + block], dst_ref=kv_in.at[block], send_sem=h_ss.at[block], recv_sem=h_rs.at[block],
            device_id={'cpo': next_core, 'cpi': next_chip}, device_id_type=MESH)

    def o_send(block):
        return pltpu.make_async_remote_copy(
            src_ref=o_out.at[block], dst_ref=o_in.at[my_head], send_sem=o_ss.at[block], recv_sem=o_rs.at[my_head],
            device_id={'cpi': base + block}, device_id_type=MESH)

    def o_recv(head):
        return pltpu.make_async_remote_copy(
            src_ref=o_in.at[head], dst_ref=o_in.at[head], send_sem=o_ss.at[0], recv_sem=o_rs.at[head],
            device_id={'cpi': base + member_of(head)}, device_id_type=MESH)

    my_y = me // 4

    def kv_chunk(c, carry):
        pltpu.make_async_copy(wk_hbm.at[:, pl.ds(0, 8), :], w0, w_sem.at[0]).wait()
        k_all = project(w0)
        for i in range(8):
            kv_out[8 * c + i, 0:TOK, :] = rope(k_all[:, HD * i:HD * i + HD]).astype(jnp.bfloat16)

        @pl.when(c == 0)
        def _():
            pltpu.make_async_copy(wk_hbm.at[:, pl.ds(8, 8), :], w0, w_sem.at[0]).start()

        @pl.when(c == 1)
        def _():
            pltpu.make_async_copy(wq_hbm.at[:, pl.ds(0, 8), :], w0, w_sem.at[0]).start()

        pltpu.make_async_copy(wv_hbm.at[:, pl.ds(0, 8), :], w1, w_sem.at[1]).wait()
        v_all = project(w1)
        for i in range(8):
            v_bf = v_all[:, HD * i:HD * i + HD].astype(jnp.bfloat16)
            kv_out[8 * c + i, TOK:TOK + HD, :] = v_bf[0:HD].T
            kv_out[8 * c + i, TOK + HD:TOK + 2 * HD, :] = v_bf[HD:TOK].T

        @pl.when(c == 0)
        def _():
            pltpu.make_async_copy(wv_hbm.at[:, pl.ds(8, 8), :], w1, w_sem.at[1]).start()

        @pl.when(c == 1)
        def _():
            pltpu.make_async_copy(wq_hbm.at[:, pl.ds(8, 8), :], w1, w_sem.at[1]).start()

        for step in range(4):
            for b in range(2):
                head = 8 * c + 4 * b + (my_y + step) % 4

                @pl.when(head != my_head)
                def _():
                    kv_send(head).start()
        return carry

    lax.fori_loop(0, 2, kv_chunk, 0)

    def q_half(slot_ref, j):
        q_all = project(slot_ref)
        for i in range(4):
            for g in range(2):
                lo = HD * (2 * i + g)
                q_out[4 * j + i, TOK * g:TOK * g + TOK, :] = rope(q_all[:, lo:lo + HD]).astype(jnp.bfloat16)

    def q_sends(j):
        for step in range(4):
            head = 4 * j + (my_y + step) % 4

            @pl.when(head != my_head)
            def _():
                q_send(head).start()

    def q_chunk(c, carry):
        pltpu.make_async_copy(wq_hbm.at[:, pl.ds(0, 8), :], w0, w_sem.at[0]).wait()
        q_half(w0, 2 * c)

        @pl.when(c == 0)
        def _():
            pltpu.make_async_copy(wq_hbm.at[:, pl.ds(16, 8), :], w0, w_sem.at[0]).start()

        q_sends(2 * c)
        pltpu.make_async_copy(wq_hbm.at[:, pl.ds(0, 8), :], w1, w_sem.at[1]).wait()
        q_half(w1, 2 * c + 1)

        @pl.when(c == 0)
        def _():
            pltpu.make_async_copy(wq_hbm.at[:, pl.ds(24, 8), :], w1, w_sem.at[1]).start()

        q_sends(2 * c + 1)
        return carry

    lax.fori_loop(0, 2, q_chunk, 0)

    n_wo = wo_buf.shape[0]

    def wo_copy(g):
        return pltpu.make_async_copy(wo_hbm.at[pl.ds(4 * g, 4)], wo_buf.at[g % n_wo], wo_sem.at[g % n_wo])

    for g in range(n_wo):
        wo_copy(g).start()

    kv_in[BACK + me] = kv_out[my_head]
    q_in[me] = q_out[my_head]

    def kv_low(step, carry):
        src = step

        @pl.when(src != me)
        def _():
            kv_recv(src).wait_recv()

        @pl.when(src >= BACK)
        def _():
            halo(src - BACK).start()
        return carry

    lax.fori_loop(0, GROUP, kv_low, 0)

    scale = HD ** -0.5 * math.log2(math.e)
    rows_k = lax.broadcasted_iota(jnp.int32, (TOK, 2 * TOK), 0)
    rows_q = lax.broadcasted_iota(jnp.int32, (TOK, 2 * TOK), 1) % TOK
    causal = rows_k <= rows_q
    is_first = (z == 0) & (core == 0)
    neg = jnp.float32(-jnp.inf)

    def scores(block, q):
        return lax.dot_general(kv_in[block, 0:TOK, :], q, (((1,), (1,)), ((), ())), preferred_element_type=jnp.float32)

    def v_of(block):
        return jnp.concatenate([kv_in[block, TOK:TOK + HD, :], kv_in[block, TOK + HD:TOK + 2 * HD, :]], axis=1)

    def attend(i):
        q = q_in[i]
        bias = [jnp.where(is_first & (i + j < BACK), neg, jnp.float32(0.0)) for j in range(BACK)]
        merged = jnp.where(causal, scores(i + BACK, q), scores(i, q) + bias[0])
        s_buf[0] = merged
        top = jnp.max(merged, axis=0, keepdims=True)
        for j in range(1, BACK):
            s = scores(i + j, q)
            s_buf[j] = s
            top = jnp.maximum(top, jnp.max(s, axis=0, keepdims=True) + bias[j])
        top = top * scale
        p = jnp.exp2(s_buf[0] * scale - top)
        total = jnp.sum(p, axis=0, keepdims=True)
        zero = jnp.zeros_like(p)
        acc = jnp.dot(v_of(i + BACK), jnp.where(causal, p, zero).astype(jnp.bfloat16), preferred_element_type=jnp.float32)
        acc += jnp.dot(v_of(i), jnp.where(causal, zero, p).astype(jnp.bfloat16), preferred_element_type=jnp.float32)
        for j in range(1, BACK):
            p = jnp.exp2(s_buf[j] * scale - (top - bias[j]))
            total += jnp.sum(p, axis=0, keepdims=True)
            acc += jnp.dot(v_of(i + j), p.astype(jnp.bfloat16), preferred_element_type=jnp.float32)
        o = (acc / total).T
        o_out[i, :, 0:HD] = o[0:TOK].astype(jnp.bfloat16)
        o_out[i, :, HD:2 * HD] = o[TOK:2 * TOK].astype(jnp.bfloat16)

    def attend_step(t, carry):
        i = jnp.where(t < 8, 8, 0) + (me + t) % 8

        @pl.when(i != me)
        def _():
            q_recv(i).wait_recv()

        @pl.when(t == 8)
        def _():
            for b in range(BACK):
                halo(b).wait_recv()

        attend(i)

        @pl.when(i != me)
        def _():
            o_send(i).start()
        return carry

    lax.fori_loop(0, GROUP, attend_step, 0)

    o_in[my_head] = o_out[me]

    def out_step(g, carry):
        wo_copy(g).wait()
        for k in range(2):
            @pl.when(2 * g + k != my_head)
            def _():
                o_recv(2 * g + k).wait_recv()
        o = jnp.concatenate([o_in[2 * g], o_in[2 * g + 1]], axis=1)
        w = wo_buf[g % n_wo].reshape(4 * HD, d_model)
        part = jnp.dot(o, w, preferred_element_type=jnp.float32)

        @pl.when(g == 0)
        def _():
            y_acc[...] = part

        @pl.when(g > 0)
        def _():
            y_acc[...] += part

        @pl.when(g + n_wo < 8)
        def _():
            wo_copy(g + n_wo).start()
        return carry

    lax.fori_loop(0, 8, out_step, 0)
    y_bf[...] = y_acc[...].astype(jnp.bfloat16)
    y_copy = pltpu.make_async_copy(y_bf, y_hbm, y_sem)
    y_copy.start()

    for b in range(BACK):
        halo(b).wait_send()

    def drain(h, carry):
        @pl.when(h != my_head)
        def _():
            kv_send(h).wait_send()
            q_send(h).wait_send()

        @pl.when(h != me)
        def _():
            o_send(h).wait_send()
        return carry

    lax.fori_loop(0, GROUP, drain, 0)
    y_copy.wait()


def solution(mesh):
    n_inner = mesh.shape['cpi']

    def local_fn(hidden, w_q, w_k, w_v, w_o):
        tok, d_model = hidden.shape
        rank = lax.axis_index('cpo') * n_inner + lax.axis_index('cpi')
        positions = (rank * tok + jnp.arange(tok)).astype(jnp.float32)
        inv_freq = ROPE_BASE ** (-jnp.arange(HD // 2, dtype=jnp.float32) * 2.0 / HD)
        angles = positions[:, None] * inv_freq
        cos_t = jnp.cos(angles)
        sin_t = jnp.sin(angles)
        cos_full = jnp.concatenate([cos_t, cos_t], axis=1)
        sin_full = jnp.concatenate([-sin_t, sin_t], axis=1)
        any_spec = pl.BlockSpec(memory_space=pl.ANY)
        bf = jnp.bfloat16
        dma = pltpu.SemaphoreType.DMA
        return pl.pallas_call(
            body,
            out_shape=jax.ShapeDtypeStruct((tok, d_model), bf),
            in_specs=[any_spec] * 7,
            out_specs=any_spec,
            scratch_shapes=[
                pltpu.VMEM((tok, d_model), bf),
                pltpu.VMEM((tok, HD), jnp.float32),
                pltpu.VMEM((tok, HD), jnp.float32),
                pltpu.VMEM((d_model, 8, HD), bf),
                pltpu.VMEM((d_model, 8, HD), bf),
                pltpu.VMEM((GROUP, 2 * TOK, HD), bf),
                pltpu.VMEM((GROUP, 2 * TOK, HD), bf),
                pltpu.VMEM((GROUP + BACK, 2 * TOK, HD), bf),
                pltpu.VMEM((GROUP, 2 * TOK, HD), bf),
                pltpu.VMEM((BACK, TOK, 2 * TOK), jnp.float32),
                pltpu.VMEM((GROUP, TOK, 2 * HD), bf),
                pltpu.VMEM((GROUP, TOK, 2 * HD), bf),
                pltpu.VMEM((2, 4, HD, d_model), bf),
                pltpu.VMEM((tok, d_model), jnp.float32),
                pltpu.VMEM((tok, d_model), bf),
                dma((3,)), dma((2,)), dma((2,)), dma(()),
                dma((GROUP,)), dma((GROUP,)), dma((BACK,)), dma((BACK,)),
                dma((GROUP,)), dma((GROUP,)), dma((GROUP,)), dma((GROUP,)),
            ],
            compiler_params=pltpu.CompilerParams(collective_id=0, has_side_effects=True, vmem_limit_bytes=67043328),
        )(hidden, w_q, w_k, w_v, w_o, cos_full, sin_full)

    return jax.shard_map(local_fn, mesh=mesh,
                         in_specs=(P(('dp', 'cpo', 'cpi'), None), P(), P(), P(), P()),
                         out_specs=P(('dp', 'cpo', 'cpi'), None), check_vma=False)
```

```python
import functools
import math

import jax
import jax.numpy as jnp
from jax import lax
from jax.experimental import pallas as pl
from jax.experimental.pallas import tpu as pltpu
from jax.sharding import PartitionSpec as P

ROPE_BASE = 10000.0
GROUP = 16
TOK = 256
HD = 128
BACK = 8
MESH = pl.DeviceIdType.MESH


def head_of(member):
    y = member // 4
    x = member % 4
    d = (x + 4 - y) % 4
    return 8 * (d % 2) + 4 * (d // 2) + y


def member_of(head):
    c = head // 8
    b = (head // 4) % 2
    y = head % 4
    return 4 * y + (y + c + 2 * b) % 4


def body(x_hbm, wq_hbm, wk_hbm, wv_hbm, wo_hbm, cos_hbm, sin_hbm, y_hbm,
         x_v, cos_v, sin_v, w0, w1, kv_out, q_out, kv_in, q_in, s_a, s_b, o_in, wo_buf, y_acc,
         in_sem, w_sem, wo_sem, y_sem, k_ss, k_rs, v_ss, v_rs, h_ss, h_rs, q_ss, q_rs, o_ss, o_rs):
    core = lax.axis_index('cpo')
    chip = lax.axis_index('cpi')
    z = chip // GROUP
    me = chip % GROUP
    base = z * GROUP
    my_y = me // 4
    my_class = (me % 4 + 4 - my_y) % 4
    my_head = head_of(me)
    d_model = x_v.shape[1]

    def eight(w_hbm, chunk):
        return w_hbm.at[:, pl.ds(pl.multiple_of(8 * chunk, 8), 8), :]

    def class_chunk(k):
        d = (my_class + k) % 4
        return 2 * (d % 2) + d // 2

    def w_load(w_hbm, chunk, slot):
        return pltpu.make_async_copy(eight(w_hbm, chunk), (w0, w1)[slot], w_sem.at[slot])

    x_copy = pltpu.make_async_copy(x_hbm, x_v, in_sem.at[0])
    cos_copy = pltpu.make_async_copy(cos_hbm, cos_v, in_sem.at[1])
    sin_copy = pltpu.make_async_copy(sin_hbm, sin_v, in_sem.at[2])
    first = my_class % 2
    x_copy.start()
    w_load(wk_hbm, first, 0).start()
    cos_copy.start()
    sin_copy.start()
    w_load(wv_hbm, first, 1).start()

    next_core = jnp.where(z == 3, 1 - core, core)
    next_chip = ((z + 1) % 4) * GROUP + me
    prev_core = jnp.where(z == 0, 1 - core, core)
    prev_chip = ((z + 3) % 4) * GROUP + me

    barrier = pltpu.get_barrier_semaphore()
    for step in range(1, GROUP):
        pl.semaphore_signal(barrier, inc=1, device_id={'cpi': base + (me + step) % GROUP}, device_id_type=MESH)
    pl.semaphore_signal(barrier, inc=1, device_id={'cpo': next_core, 'cpi': next_chip}, device_id_type=MESH)
    pl.semaphore_signal(barrier, inc=1, device_id={'cpo': prev_core, 'cpi': prev_chip}, device_id_type=MESH)
    pl.semaphore_wait(barrier, GROUP + 1)

    x_copy.wait()
    cos_copy.wait()
    sin_copy.wait()

    def project(w_ref):
        w = w_ref[...].reshape(d_model, 8 * HD)
        return jnp.dot(x_v[...], w, preferred_element_type=jnp.float32)

    def rope(u):
        return u * cos_v[...] + pltpu.roll(u, HD // 2, 1) * sin_v[...]

    k_rows = pl.ds(0, TOK)
    v_rows = pl.ds(TOK, TOK)

    def k_copy(head, dst_member, src):
        return pltpu.make_async_remote_copy(
            src_ref=kv_out.at[head, k_rows], dst_ref=kv_in.at[BACK + src, k_rows], send_sem=k_ss.at[head],
            recv_sem=k_rs.at[src], device_id={'cpi': base + dst_member}, device_id_type=MESH)

    def v_copy(head, dst_member, src):
        return pltpu.make_async_remote_copy(
            src_ref=kv_out.at[head, v_rows], dst_ref=kv_in.at[BACK + src, v_rows], send_sem=v_ss.at[head],
            recv_sem=v_rs.at[src], device_id={'cpi': base + dst_member}, device_id_type=MESH)

    def q_copy(head, dst_member, src):
        return pltpu.make_async_remote_copy(
            src_ref=q_out.at[head], dst_ref=q_in.at[src], send_sem=q_ss.at[head], recv_sem=q_rs.at[src],
            device_id={'cpi': base + dst_member}, device_id_type=MESH)

    def o_copy(block, head):
        return pltpu.make_async_remote_copy(
            src_ref=kv_out.at[block], dst_ref=o_in.at[head], send_sem=o_ss.at[block], recv_sem=o_rs.at[head],
            device_id={'cpi': base + block}, device_id_type=MESH)

    def halo(block):
        return pltpu.make_async_remote_copy(
            src_ref=kv_in.at[GROUP + block], dst_ref=kv_in.at[block], send_sem=h_ss.at[block], recv_sem=h_rs.at[block],
            device_id={'cpo': next_core, 'cpi': next_chip}, device_id_type=MESH)

    def send_class(copy, k):
        for step in range(4):
            y = (my_y + step) % 4
            head = 4 * class_chunk(k) + y

            def go(head=head):
                copy(head, member_of(head), me).start()

            if step == 0:
                pl.when(k > 0)(go)
            else:
                go()

    def kv_chunk(t, carry):
        c = (first + t) % 2
        w_load(wk_hbm, 0, 0).wait()
        k_all = project(w0)
        for i in range(8):
            kv_out[8 * c + i, 0:TOK, :] = rope(k_all[:, HD * i:HD * i + HD]).astype(jnp.bfloat16)

        @pl.when(t == 0)
        def _():
            w_load(wk_hbm, 1 - first, 0).start()

        @pl.when(t == 1)
        def _():
            w_load(wq_hbm, class_chunk(0), 0).start()

        send_class(k_copy, t)
        send_class(k_copy, t + 2)

        w_load(wv_hbm, 0, 1).wait()
        v_all = project(w1)
        for i in range(8):
            v_bf = v_all[:, HD * i:HD * i + HD].astype(jnp.bfloat16)
            kv_out[8 * c + i, TOK:TOK + HD, :] = v_bf[0:HD].T
            kv_out[8 * c + i, TOK + HD:TOK + 2 * HD, :] = v_bf[HD:TOK].T

        @pl.when(t == 0)
        def _():
            w_load(wv_hbm, 1 - first, 1).start()

        @pl.when(t == 1)
        def _():
            w_load(wq_hbm, class_chunk(1), 1).start()

        send_class(v_copy, t)
        send_class(v_copy, t + 2)
        return carry

    lax.fori_loop(0, 2, kv_chunk, 0)
    kv_in[BACK + me] = kv_out[my_head]

    def wait_kv(src):
        @pl.when(src != me)
        def _():
            k_copy(0, 0, src).wait_recv()
            v_copy(0, 0, src).wait_recv()

    def forward(parity):
        for i in range(4):
            y = 2 + i // 2
            src = 4 * y + (y + my_class + parity + 2 * (i % 2)) % 4
            wait_kv(src)
            halo(src - BACK).start()

    def q_store(slot_ref, k):
        q_all = project(slot_ref)
        j = class_chunk(k)
        for i in range(4):
            for g in range(2):
                lo = HD * (2 * i + g)
                q_out[4 * j + i, TOK * g:TOK * g + TOK, :] = rope(q_all[:, lo:lo + HD]).astype(jnp.bfloat16)

    def q_chunk(u, carry):
        for half in range(2):
            k = 2 * u + half
            w_load(wq_hbm, 0, half).wait()
            q_store((w0, w1)[half], k)

            @pl.when(u == 0)
            def _():
                w_load(wq_hbm, class_chunk(2 + half), half).start()

            send_class(q_copy, k)
        forward(u)
        return carry

    lax.fori_loop(0, 2, q_chunk, 0)

    n_wo = wo_buf.shape[0]

    def out_head(g):
        return 4 * class_chunk(g // 2) + 2 * (g % 2)

    def wo_copy(g):
        return pltpu.make_async_copy(wo_hbm.at[pl.ds(2 * out_head(g), 4)], wo_buf.at[g % n_wo], wo_sem.at[g % n_wo])

    for g in range(n_wo):
        wo_copy(g).start()

    q_in[me] = q_out[my_head]

    def kv_low(src, carry):
        wait_kv(src)
        return carry

    lax.fori_loop(0, BACK, kv_low, 0)

    def kv_drain(h, carry):
        @pl.when(h != my_head)
        def _():
            k_copy(h, 0, 0).wait_send()
            v_copy(h, 0, 0).wait_send()
        return carry

    lax.fori_loop(0, GROUP, kv_drain, 0)

    scale = HD ** -0.5 * math.log2(math.e)
    rows_k = lax.broadcasted_iota(jnp.int32, (TOK, 2 * TOK), 0)
    rows_q = lax.broadcasted_iota(jnp.int32, (TOK, 2 * TOK), 1) % TOK
    causal = rows_k <= rows_q
    is_first = (z == 0) & (core == 0)
    neg = jnp.float32(-jnp.inf)

    def biases(i):
        return [jnp.where(is_first & (i + j < BACK), neg, jnp.float32(0.0)) for j in range(BACK)]

    def scores(block, q):
        return lax.dot_general(kv_in[block, 0:TOK, :], q, (((1,), (1,)), ((), ())), preferred_element_type=jnp.float32)

    def v_of(block):
        return jnp.concatenate([kv_in[block, TOK:TOK + HD, :], kv_in[block, TOK + HD:TOK + 2 * HD, :]], axis=1)

    def score_tile(buf, i, q, j, bias, top):
        if j == 0:
            s = jnp.where(causal, scores(i + BACK, q), scores(i, q) + bias[0])
            buf[0] = s
            return jnp.max(s, axis=0, keepdims=True)
        s = scores(i + j, q)
        buf[j] = s
        return jnp.maximum(top, jnp.max(s, axis=0, keepdims=True) + bias[j])

    def pv_tile(buf, i, j, bias, top, total, acc):
        if j == 0:
            p = jnp.exp2(buf[0] * scale - top)
            zero = jnp.zeros_like(p)
            acc = jnp.dot(v_of(i + BACK), jnp.where(causal, p, zero).astype(jnp.bfloat16),
                          preferred_element_type=jnp.float32)
            acc += jnp.dot(v_of(i), jnp.where(causal, zero, p).astype(jnp.bfloat16),
                           preferred_element_type=jnp.float32)
            return jnp.sum(p, axis=0, keepdims=True), acc
        p = jnp.exp2(buf[j] * scale - (top - bias[j]))
        total = total + jnp.sum(p, axis=0, keepdims=True)
        return total, acc + jnp.dot(v_of(i + j), p.astype(jnp.bfloat16), preferred_element_type=jnp.float32)

    def stage(done, ahead):
        if ahead is not None:
            buf_n, i_n = ahead
            q = q_in[i_n]
            bias_n = biases(i_n)
        if done is not None:
            buf_d, i_d, top_d = done
            top_d = top_d * scale
            bias_d = biases(i_d)
        top_n = total = acc = None
        for j in range(BACK):
            if ahead is not None:
                top_n = score_tile(buf_n, i_n, q, j, bias_n, top_n)
            if done is not None:
                total, acc = pv_tile(buf_d, i_d, j, bias_d, top_d, total, acc)
        if done is not None:
            o = (acc / total).T
            kv_out[i_d] = o.astype(jnp.bfloat16)
        return top_n

    def out_step(g, carry):
        wo_copy(g).wait()
        head = out_head(g)
        for k in range(2):
            @pl.when(head + k != my_head)
            def _():
                o_copy(0, head + k).wait_recv()
        o = jnp.concatenate([o_in[head + k, TOK * g2:TOK * g2 + TOK] for k in range(2) for g2 in range(2)], axis=1)
        w = wo_buf[g % n_wo].reshape(4 * HD, d_model)
        part = jnp.dot(o, w, preferred_element_type=jnp.float32)

        @pl.when(g == 0)
        def _():
            y_acc[...] = part

        @pl.when(g > 0)
        def _():
            y_acc[...] += part

        @pl.when(g + n_wo < 8)
        def _():
            wo_copy(g + n_wo).start()
        return carry

    def attend_set(t, carry):
        blocks = []
        for n in range(4):
            y = (2 if n < 2 else 0) + (my_y + n) % 2
            blocks.append(4 * y + (y + my_class + 4 - t) % 4)
        bufs = (s_a, s_b, s_a, s_b)

        def wait_q(i):
            @pl.when(i != me)
            def _():
                q_copy(0, 0, i).wait_recv()

        def ship(i):
            @pl.when(i != me)
            def _():
                o_copy(i, my_head).start()

            @pl.when(i == me)
            def _():
                o_in[my_head] = kv_out[me]

        wait_q(blocks[0])
        top = stage(None, (bufs[0], blocks[0]))
        for n in range(4):
            if n == 1:
                @pl.when(t == 0)
                def _():
                    for b in range(BACK):
                        halo(b).wait_recv()
            if n < 3:
                wait_q(blocks[n + 1])
            top = stage((bufs[n], blocks[n], top), (bufs[n + 1], blocks[n + 1]) if n < 3 else None)
            ship(blocks[n])

        @pl.when(t > 0)
        def _():
            lax.fori_loop(2 * t - 2, 2 * t, out_step, 0)
        return carry

    lax.fori_loop(0, 4, attend_set, 0)
    lax.fori_loop(6, 8, out_step, 0)

    rows = TOK // 4
    y_copies = []
    for r in range(4):
        part = pl.ds(rows * r, rows)
        x_v[part, :] = y_acc[part, :].astype(jnp.bfloat16)
        y_copies.append(pltpu.make_async_copy(x_v.at[part], y_hbm.at[part], y_sem.at[r]))
    for y_copy in y_copies:
        y_copy.start()

    for b in range(BACK):
        halo(b).wait_send()

    def drain(h, carry):
        @pl.when(h != my_head)
        def _():
            q_copy(h, 0, 0).wait_send()

        @pl.when(h != me)
        def _():
            o_copy(h, 0).wait_send()
        return carry

    lax.fori_loop(0, GROUP, drain, 0)
    for y_copy in y_copies:
        y_copy.wait()


def solution(mesh):
    n_inner = mesh.shape['cpi']

    def local_fn(hidden, w_q, w_k, w_v, w_o):
        tok, d_model = hidden.shape
        rank = lax.axis_index('cpo') * n_inner + lax.axis_index('cpi')
        positions = (rank * tok + jnp.arange(tok)).astype(jnp.float32)
        inv_freq = ROPE_BASE ** (-jnp.arange(HD // 2, dtype=jnp.float32) * 2.0 / HD)
        angles = positions[:, None] * inv_freq
        cos_t = jnp.cos(angles)
        sin_t = jnp.sin(angles)
        cos_full = jnp.concatenate([cos_t, cos_t], axis=1)
        sin_full = jnp.concatenate([-sin_t, sin_t], axis=1)
        any_spec = pl.BlockSpec(memory_space=pl.ANY)
        bf = jnp.bfloat16
        dma = pltpu.SemaphoreType.DMA
        return pl.pallas_call(
            body,
            out_shape=jax.ShapeDtypeStruct((tok, d_model), bf),
            in_specs=[any_spec] * 7,
            out_specs=any_spec,
            scratch_shapes=[
                pltpu.VMEM((tok, d_model), bf),
                pltpu.VMEM((tok, HD), jnp.float32),
                pltpu.VMEM((tok, HD), jnp.float32),
                pltpu.VMEM((d_model, 8, HD), bf),
                pltpu.VMEM((d_model, 8, HD), bf),
                pltpu.VMEM((GROUP, 2 * TOK, HD), bf),
                pltpu.VMEM((GROUP, 2 * TOK, HD), bf),
                pltpu.VMEM((GROUP + BACK, 2 * TOK, HD), bf),
                pltpu.VMEM((GROUP, 2 * TOK, HD), bf),
                pltpu.VMEM((BACK, TOK, 2 * TOK), jnp.float32),
                pltpu.VMEM((BACK, TOK, 2 * TOK), jnp.float32),
                pltpu.VMEM((GROUP, 2 * TOK, HD), bf),
                pltpu.VMEM((2, 4, HD, d_model), bf),
                pltpu.VMEM((tok, d_model), jnp.float32),
                dma((3,)), dma((2,)), dma((2,)), dma((4,)),
                dma((GROUP,)), dma((GROUP,)), dma((GROUP,)), dma((GROUP,)), dma((BACK,)), dma((BACK,)),
                dma((GROUP,)), dma((GROUP,)), dma((GROUP,)), dma((GROUP,)),
            ],
            compiler_params=pltpu.CompilerParams(collective_id=0, has_side_effects=True, vmem_limit_bytes=67043328),
        )(hidden, w_q, w_k, w_v, w_o, cos_full, sin_full)

    return jax.shard_map(local_fn, mesh=mesh,
                         in_specs=(P(('dp', 'cpo', 'cpi'), None), P(), P(), P(), P()),
                         out_specs=P(('dp', 'cpo', 'cpi'), None), check_vma=False)
```

```python
import functools
import math

import jax
import jax.numpy as jnp
import numpy as np
from jax import lax
from jax.experimental import pallas as pl
from jax.experimental.pallas import tpu as pltpu
from jax.sharding import PartitionSpec as P

ROPE_BASE = 10000.0
GROUP = 16
TOK = 256
HD = 128
BACK = 8
MESH = pl.DeviceIdType.MESH


def head_of(member):
    y = member // 4
    x = member % 4
    d = (x + 4 - y) % 4
    return 8 * (d % 2) + 4 * (d // 2) + y


def member_of(head):
    c = head // 8
    b = (head // 4) % 2
    y = head % 4
    return 4 * y + (y + c + 2 * b) % 4


def body(x_hbm, wq_hbm, wk_hbm, wv_hbm, wo_hbm, freq_hbm, y_hbm,
         x_v, freq_v, cos_v, sin_v, w0, w1, kv_out, q_out, kv_in, q_in, s_a, s_b, o_in, wo_buf, y_acc,
         in_sem, w_sem, wo_sem, y_sem, k_ss, k_rs, v_ss, v_rs, h_ss, h_rs, q_ss, q_rs, o_ss, o_rs):
    core = lax.axis_index('cpo')
    chip = lax.axis_index('cpi')
    z = chip // GROUP
    me = chip % GROUP
    base = z * GROUP
    my_y = me // 4
    my_class = (me % 4 + 4 - my_y) % 4
    my_head = head_of(me)
    d_model = x_v.shape[1]

    def class_chunk(k):
        d = (my_class + k) % 4
        return 2 * (d % 2) + d // 2

    half_d = d_model // 2

    def w_half(w_hbm, chunk, slot, part):
        rows = pl.ds(half_d * part, half_d)
        src = w_hbm.at[rows, pl.ds(pl.multiple_of(8 * chunk, 8), 8), :]
        return pltpu.make_async_copy(src, (w0, w1)[slot].at[rows], w_sem.at[slot, part])

    def w_start(w_hbm, chunk, slot):
        for part in range(2):
            w_half(w_hbm, chunk, slot, part).start()

    def x_half(part):
        cols = pl.ds(half_d * part, half_d)
        return pltpu.make_async_copy(x_hbm.at[:, cols], x_v.at[:, cols], in_sem.at[part])

    freq_copy = pltpu.make_async_copy(freq_hbm, freq_v, in_sem.at[2])
    first = my_class % 2
    freq_copy.start()
    for part in range(2):
        x_half(part).start()
        w_half(wk_hbm, first, 0, part).start()
    w_start(wv_hbm, first, 1)

    next_core = jnp.where(z == 3, 1 - core, core)
    next_chip = ((z + 1) % 4) * GROUP + me
    prev_core = jnp.where(z == 0, 1 - core, core)
    prev_chip = ((z + 3) % 4) * GROUP + me

    barrier = pltpu.get_barrier_semaphore()
    for step in range(1, GROUP):
        pl.semaphore_signal(barrier, inc=1, device_id={'cpi': base + (me + step) % GROUP}, device_id_type=MESH)
    pl.semaphore_signal(barrier, inc=1, device_id={'cpo': next_core, 'cpi': next_chip}, device_id_type=MESH)
    pl.semaphore_signal(barrier, inc=1, device_id={'cpo': prev_core, 'cpi': prev_chip}, device_id_type=MESH)

    freq_copy.wait()
    pos = (core * (4 * GROUP) + chip) * TOK + lax.broadcasted_iota(jnp.int32, (TOK, HD), 0)
    angle = pos.astype(jnp.float32) * freq_v[...]
    low = lax.broadcasted_iota(jnp.int32, (TOK, HD), 1) < HD // 2
    cos_v[...] = jnp.cos(angle)
    sin_t = jnp.sin(angle)
    sin_v[...] = jnp.where(low, -sin_t, sin_t)

    pl.semaphore_wait(barrier, GROUP + 1)
    x_half(0).wait()
    x_half(1).wait()

    def project(slot):
        w_ref = (w0, w1)[slot]
        cols = slice(8 * HD * slot, 8 * HD * slot + 8 * HD)
        for part in range(2):
            w_half(wk_hbm, 0, slot, part).wait()
            w = w_ref[half_d * part:half_d * part + half_d].reshape(half_d, 8 * HD)
            term = jnp.dot(x_v[:, half_d * part:half_d * part + half_d], w, preferred_element_type=jnp.float32)
            if part == 0:
                y_acc[:, cols] = term
        return y_acc[:, cols] + term

    def rope(u):
        return u * cos_v[...] + pltpu.roll(u, HD // 2, 1) * sin_v[...]

    k_rows = pl.ds(0, TOK)
    v_rows = pl.ds(TOK, TOK)

    def k_copy(head, dst_member, src):
        return pltpu.make_async_remote_copy(
            src_ref=kv_out.at[head, k_rows], dst_ref=kv_in.at[BACK + src, k_rows], send_sem=k_ss.at[head],
            recv_sem=k_rs.at[src], device_id={'cpi': base + dst_member}, device_id_type=MESH)

    def v_copy(head, dst_member, src):
        return pltpu.make_async_remote_copy(
            src_ref=kv_out.at[head, v_rows], dst_ref=kv_in.at[BACK + src, v_rows], send_sem=v_ss.at[head],
            recv_sem=v_rs.at[src], device_id={'cpi': base + dst_member}, device_id_type=MESH)

    def q_copy(head, dst_member, src):
        return pltpu.make_async_remote_copy(
            src_ref=q_out.at[head], dst_ref=q_in.at[src], send_sem=q_ss.at[head], recv_sem=q_rs.at[src],
            device_id={'cpi': base + dst_member}, device_id_type=MESH)

    def o_copy(block, head):
        return pltpu.make_async_remote_copy(
            src_ref=kv_out.at[block], dst_ref=o_in.at[head], send_sem=o_ss.at[block], recv_sem=o_rs.at[head],
            device_id={'cpi': base + block}, device_id_type=MESH)

    def halo(block):
        return pltpu.make_async_remote_copy(
            src_ref=kv_in.at[GROUP + block], dst_ref=kv_in.at[block], send_sem=h_ss.at[block], recv_sem=h_rs.at[block],
            device_id={'cpo': next_core, 'cpi': next_chip}, device_id_type=MESH)

    def send_class(copy, k):
        for step in range(4):
            y = (my_y + step) % 4
            head = 4 * class_chunk(k) + y

            def go(head=head):
                copy(head, member_of(head), me).start()

            if step == 0:
                pl.when(k > 0)(go)
            else:
                go()

    def kv_chunk(t, carry):
        c = (first + t) % 2
        k_all = project(0)
        for i in range(8):
            kv_out[8 * c + i, 0:TOK, :] = rope(k_all[:, HD * i:HD * i + HD]).astype(jnp.bfloat16)

        @pl.when(t == 0)
        def _():
            w_start(wk_hbm, 1 - first, 0)

        @pl.when(t == 1)
        def _():
            w_start(wq_hbm, class_chunk(0), 0)

        send_class(k_copy, t)
        send_class(k_copy, t + 2)

        v_all = project(1)
        for i in range(8):
            v_bf = v_all[:, HD * i:HD * i + HD].astype(jnp.bfloat16)
            kv_out[8 * c + i, TOK:TOK + HD, :] = v_bf[0:HD].T
            kv_out[8 * c + i, TOK + HD:TOK + 2 * HD, :] = v_bf[HD:TOK].T

        @pl.when(t == 0)
        def _():
            w_start(wv_hbm, 1 - first, 1)

        @pl.when(t == 1)
        def _():
            w_start(wq_hbm, class_chunk(1), 1)

        send_class(v_copy, t)
        send_class(v_copy, t + 2)
        return carry

    lax.fori_loop(0, 2, kv_chunk, 0)
    kv_in[BACK + me] = kv_out[my_head]

    def wait_kv(src):
        @pl.when(src != me)
        def _():
            k_copy(0, 0, src).wait_recv()
            v_copy(0, 0, src).wait_recv()

    def forward(parity):
        for i in range(4):
            y = 2 + i // 2
            src = 4 * y + (y + my_class + parity + 2 * (i % 2)) % 4
            wait_kv(src)
            halo(src - BACK).start()

    def q_store(slot, k):
        q_all = project(slot)
        j = class_chunk(k)
        for i in range(4):
            for g in range(2):
                lo = HD * (2 * i + g)
                q_out[4 * j + i, TOK * g:TOK * g + TOK, :] = rope(q_all[:, lo:lo + HD]).astype(jnp.bfloat16)

    def q_chunk(u, carry):
        for half in range(2):
            k = 2 * u + half
            q_store(half, k)

            @pl.when(u == 0)
            def _():
                w_start(wq_hbm, class_chunk(2 + half), half)

            send_class(q_copy, k)

            @pl.when(u == half)
            def _():
                forward(half)
        return carry

    lax.fori_loop(0, 2, q_chunk, 0)

    y_acc[...] = jnp.zeros_like(y_acc)
    n_wo = wo_buf.shape[0]

    def out_head(g):
        return 4 * class_chunk(g // 2) + 2 * (g % 2)

    def wo_copy(g):
        return pltpu.make_async_copy(wo_hbm.at[pl.ds(2 * out_head(g), 4)], wo_buf.at[g % n_wo], wo_sem.at[g % n_wo])

    for g in range(n_wo):
        wo_copy(g).start()

    q_in[me] = q_out[my_head]

    def kv_low(src, carry):
        wait_kv(src)
        return carry

    lax.fori_loop(0, BACK, kv_low, 0)

    def kv_drain(h, carry):
        @pl.when(h != my_head)
        def _():
            k_copy(h, 0, 0).wait_send()
            v_copy(h, 0, 0).wait_send()
        return carry

    lax.fori_loop(0, GROUP, kv_drain, 0)

    scale = HD ** -0.5 * math.log2(math.e)
    rows_k = lax.broadcasted_iota(jnp.int32, (TOK, 2 * TOK), 0)
    rows_q = lax.broadcasted_iota(jnp.int32, (TOK, 2 * TOK), 1) % TOK
    causal = rows_k <= rows_q
    is_first = (z == 0) & (core == 0)
    neg = jnp.float32(-jnp.inf)

    def biases(i):
        return [jnp.where(is_first & (i + j < BACK), neg, jnp.float32(0.0)) for j in range(BACK)]

    def scores(block, q):
        return lax.dot_general(kv_in[block, 0:TOK, :], q, (((1,), (1,)), ((), ())), preferred_element_type=jnp.float32)

    def v_of(block):
        return jnp.concatenate([kv_in[block, TOK:TOK + HD, :], kv_in[block, TOK + HD:TOK + 2 * HD, :]], axis=1)

    def score_tile(buf, i, q, j, bias, top):
        if j == 0:
            s = jnp.where(causal, scores(i + BACK, q), scores(i, q) + bias[0])
            buf[0] = s
            return jnp.max(s, axis=0, keepdims=True)
        s = scores(i + j, q)
        buf[j] = s
        return jnp.maximum(top, jnp.max(s, axis=0, keepdims=True) + bias[j])

    def pv_tile(buf, i, j, bias, top, total, acc):
        if j == 0:
            p = jnp.exp2(buf[0] * scale - top)
            zero = jnp.zeros_like(p)
            acc = jnp.dot(v_of(i + BACK), jnp.where(causal, p, zero).astype(jnp.bfloat16),
                          preferred_element_type=jnp.float32)
            acc += jnp.dot(v_of(i), jnp.where(causal, zero, p).astype(jnp.bfloat16),
                           preferred_element_type=jnp.float32)
            return jnp.sum(p, axis=0, keepdims=True), acc
        p = jnp.exp2(buf[j] * scale - (top - bias[j]))
        total = total + jnp.sum(p, axis=0, keepdims=True)
        return total, acc + jnp.dot(v_of(i + j), p.astype(jnp.bfloat16), preferred_element_type=jnp.float32)

    def stage(done, ahead):
        if ahead is not None:
            buf_n, i_n = ahead
            q = q_in[i_n]
            bias_n = biases(i_n)
        if done is not None:
            buf_d, i_d, top_d = done
            top_d = top_d * scale
            bias_d = biases(i_d)
        top_n = total = acc = None
        for j in range(BACK):
            if ahead is not None:
                top_n = score_tile(buf_n, i_n, q, j, bias_n, top_n)
            if done is not None:
                total, acc = pv_tile(buf_d, i_d, j, bias_d, top_d, total, acc)
        if done is not None:
            o = (acc / total).T
            kv_out[i_d] = o.astype(jnp.bfloat16)
        return top_n

    n_cols = d_model // 4

    def out_rows(head):
        return jnp.concatenate([o_in[head + k, TOK * g2:TOK * g2 + TOK] for k in range(2) for g2 in range(2)], axis=1)

    def out_ready(g):
        wo_copy(g).wait()
        head = out_head(g)
        for k in range(2):
            @pl.when(head + k != my_head)
            def _():
                o_copy(0, head + k).wait_recv()
        return head

    def out_step(g, carry):
        head = out_ready(g)
        o = out_rows(head)
        w = wo_buf[g % n_wo].reshape(4 * HD, d_model)
        for n in range(4):
            cols = slice(n_cols * n, n_cols * n + n_cols)
            y_acc[:, cols] += jnp.dot(o, w[:, cols], preferred_element_type=jnp.float32)

        @pl.when(g + n_wo < 8)
        def _():
            wo_copy(g + n_wo).start()
        return carry

    def out_last():
        head = out_ready(7)
        o = out_rows(head)
        w = wo_buf[7 % n_wo].reshape(4 * HD, d_model)
        copies = []
        for n in range(4):
            cols = slice(n_cols * n, n_cols * n + n_cols)
            y = y_acc[:, cols] + jnp.dot(o, w[:, cols], preferred_element_type=jnp.float32)
            x_v[:, cols] = y.astype(jnp.bfloat16)
            part = pl.ds(n_cols * n, n_cols)
            copies.append(pltpu.make_async_copy(x_v.at[:, part], y_hbm.at[:, part], y_sem.at[n]))
            copies[-1].start()
        return copies

    def attend_set(t, carry):
        blocks = []
        for n in range(4):
            y = (2 if n < 2 else 0) + (my_y + n) % 2
            blocks.append(4 * y + (y + my_class + 4 - t) % 4)
        bufs = (s_a, s_b, s_a, s_b)

        def wait_q(i):
            @pl.when(i != me)
            def _():
                q_copy(0, 0, i).wait_recv()

        def ship(i):
            @pl.when(i != me)
            def _():
                o_copy(i, my_head).start()

            @pl.when(i == me)
            def _():
                o_in[my_head] = kv_out[me]

        wait_q(blocks[0])
        top = stage(None, (bufs[0], blocks[0]))
        for n in range(4):
            if n == 1:
                @pl.when(t == 0)
                def _():
                    for b in range(BACK):
                        halo(b).wait_recv()
            if n < 3:
                wait_q(blocks[n + 1])
            top = stage((bufs[n], blocks[n], top), (bufs[n + 1], blocks[n + 1]) if n < 3 else None)
            ship(blocks[n])

        @pl.when(t > 0)
        def _():
            lax.fori_loop(2 * t - 2, 2 * t, out_step, 0)
        return carry

    lax.fori_loop(0, 4, attend_set, 0)
    lax.fori_loop(6, 8, out_step, 0)
    y_copies = []
    for r in range(4):
        part = pl.ds(TOK // 4 * r, TOK // 4)
        x_v[part, :] = y_acc[part, :].astype(jnp.bfloat16)
        y_copies.append(pltpu.make_async_copy(x_v.at[part], y_hbm.at[part], y_sem.at[r]))
        y_copies[-1].start()

    for b in range(BACK):
        halo(b).wait_send()

    def drain(h, carry):
        @pl.when(h != my_head)
        def _():
            q_copy(h, 0, 0).wait_send()

        @pl.when(h != me)
        def _():
            o_copy(h, 0).wait_send()
        return carry

    lax.fori_loop(0, GROUP, drain, 0)
    for y_copy in y_copies:
        y_copy.wait()


def solution(mesh):
    n_inner = mesh.shape['cpi']

    def local_fn(hidden, w_q, w_k, w_v, w_o):
        tok, d_model = hidden.shape
        inv_freq = ROPE_BASE ** (-np.arange(HD // 2) * 2.0 / HD)
        freq = jnp.asarray(np.tile(np.concatenate([inv_freq, inv_freq])[None, :], (tok, 1)), jnp.float32)
        any_spec = pl.BlockSpec(memory_space=pl.ANY)
        bf = jnp.bfloat16
        dma = pltpu.SemaphoreType.DMA
        return pl.pallas_call(
            body,
            out_shape=jax.ShapeDtypeStruct((tok, d_model), bf),
            in_specs=[any_spec] * 6,
            out_specs=any_spec,
            scratch_shapes=[
                pltpu.VMEM((tok, d_model), bf),
                pltpu.VMEM((tok, HD), jnp.float32),
                pltpu.VMEM((tok, HD), jnp.float32),
                pltpu.VMEM((tok, HD), jnp.float32),
                pltpu.VMEM((d_model, 8, HD), bf),
                pltpu.VMEM((d_model, 8, HD), bf),
                pltpu.VMEM((GROUP, 2 * TOK, HD), bf),
                pltpu.VMEM((GROUP, 2 * TOK, HD), bf),
                pltpu.VMEM((GROUP + BACK, 2 * TOK, HD), bf),
                pltpu.VMEM((GROUP, 2 * TOK, HD), bf),
                pltpu.VMEM((BACK, TOK, 2 * TOK), jnp.float32),
                pltpu.VMEM((BACK, TOK, 2 * TOK), jnp.float32),
                pltpu.VMEM((GROUP, 2 * TOK, HD), bf),
                pltpu.VMEM((2, 4, HD, d_model), bf),
                pltpu.VMEM((tok, d_model), jnp.float32),
                dma((3,)), dma((2, 2)), dma((2,)), dma((4,)),
                dma((GROUP,)), dma((GROUP,)), dma((GROUP,)), dma((GROUP,)), dma((BACK,)), dma((BACK,)),
                dma((GROUP,)), dma((GROUP,)), dma((GROUP,)), dma((GROUP,)),
            ],
            compiler_params=pltpu.CompilerParams(collective_id=0, has_side_effects=True, vmem_limit_bytes=67043328),
        )(hidden, w_q, w_k, w_v, w_o, freq)

    return jax.shard_map(local_fn, mesh=mesh,
                         in_specs=(P(('dp', 'cpo', 'cpi'), None), P(), P(), P(), P()),
                         out_specs=P(('dp', 'cpo', 'cpi'), None), check_vma=False)
```

```python
import functools
import math

import jax
import jax.numpy as jnp
import numpy as np
from jax import lax
from jax.experimental import pallas as pl
from jax.experimental.pallas import tpu as pltpu
from jax.sharding import PartitionSpec as P

ROPE_BASE = 10000.0
GROUP = 16
TOK = 256
HD = 128
BACK = 8
MESH = pl.DeviceIdType.MESH


def head_of(member):
    y = member // 4
    x = member % 4
    d = (x + 4 - y) % 4
    return 8 * (d % 2) + 4 * (d // 2) + y


def member_of(head):
    c = head // 8
    b = (head // 4) % 2
    y = head % 4
    return 4 * y + (y + c + 2 * b) % 4


def body(x_hbm, wq_hbm, wk_hbm, wv_hbm, wo_hbm, freq_hbm, y_hbm,
         x_v, freq_v, cos_v, sin_v, w0, w1, kv_out, q_out, kv_in, q_in, s_a, s_b, o_in, wo_buf, y_acc,
         in_sem, w_sem, wo_sem, y_sem, k_ss, k_rs, v_ss, v_rs, h_ss, h_rs, q_ss, q_rs, o_ss, o_rs):
    core = lax.axis_index('cpo')
    chip = lax.axis_index('cpi')
    z = chip // GROUP
    me = chip % GROUP
    base = z * GROUP
    my_y = me // 4
    my_class = (me % 4 + 4 - my_y) % 4
    my_head = head_of(me)
    d_model = x_v.shape[1]

    def class_chunk(k):
        d = (my_class + k) % 4
        return 2 * (d % 2) + d // 2

    half_d = d_model // 2

    def w_half(w_hbm, chunk, slot, part):
        rows = pl.ds(half_d * part, half_d)
        src = w_hbm.at[rows, pl.ds(pl.multiple_of(8 * chunk, 8), 8), :]
        return pltpu.make_async_copy(src, (w0, w1)[slot].at[rows], w_sem.at[slot, part])

    def w_start(w_hbm, chunk, slot):
        for part in range(2):
            w_half(w_hbm, chunk, slot, part).start()

    def x_half(part):
        cols = pl.ds(half_d * part, half_d)
        return pltpu.make_async_copy(x_hbm.at[:, cols], x_v.at[:, cols], in_sem.at[part])

    freq_copy = pltpu.make_async_copy(freq_hbm, freq_v, in_sem.at[2])
    first = my_class % 2
    freq_copy.start()
    for part in range(2):
        x_half(part).start()
        w_half(wk_hbm, first, 0, part).start()
    w_start(wv_hbm, first, 1)

    next_core = jnp.where(z == 3, 1 - core, core)
    next_chip = ((z + 1) % 4) * GROUP + me
    prev_core = jnp.where(z == 0, 1 - core, core)
    prev_chip = ((z + 3) % 4) * GROUP + me

    barrier = pltpu.get_barrier_semaphore()
    for step in range(1, GROUP):
        pl.semaphore_signal(barrier, inc=1, device_id={'cpi': base + (me + step) % GROUP}, device_id_type=MESH)
    pl.semaphore_signal(barrier, inc=1, device_id={'cpo': next_core, 'cpi': next_chip}, device_id_type=MESH)
    pl.semaphore_signal(barrier, inc=1, device_id={'cpo': prev_core, 'cpi': prev_chip}, device_id_type=MESH)

    freq_copy.wait()
    pos = (core * (4 * GROUP) + chip) * TOK + lax.broadcasted_iota(jnp.int32, (TOK, HD), 0)
    angle = pos.astype(jnp.float32) * freq_v[...]
    low = lax.broadcasted_iota(jnp.int32, (TOK, HD), 1) < HD // 2
    cos_v[...] = jnp.cos(angle)
    sin_t = jnp.sin(angle)
    sin_v[...] = jnp.where(low, -sin_t, sin_t)

    pl.semaphore_wait(barrier, GROUP + 1)
    x_half(0).wait()
    x_half(1).wait()

    def project(slot):
        w_ref = (w0, w1)[slot]
        cols = slice(8 * HD * slot, 8 * HD * slot + 8 * HD)
        for part in range(2):
            w_half(wk_hbm, 0, slot, part).wait()
            w = w_ref[half_d * part:half_d * part + half_d].reshape(half_d, 8 * HD)
            term = jnp.dot(x_v[:, half_d * part:half_d * part + half_d], w, preferred_element_type=jnp.float32)
            if part == 0:
                y_acc[:, cols] = term
        return y_acc[:, cols] + term

    def rope(u):
        return u * cos_v[...] + pltpu.roll(u, HD // 2, 1) * sin_v[...]

    k_rows = pl.ds(0, TOK)
    v_rows = pl.ds(TOK, TOK)

    def k_copy(head, dst_member, src):
        return pltpu.make_async_remote_copy(
            src_ref=kv_out.at[head, k_rows], dst_ref=kv_in.at[BACK + src, k_rows], send_sem=k_ss.at[head],
            recv_sem=k_rs.at[src], device_id={'cpi': base + dst_member}, device_id_type=MESH)

    def v_copy(head, dst_member, src):
        return pltpu.make_async_remote_copy(
            src_ref=kv_out.at[head, v_rows], dst_ref=kv_in.at[BACK + src, v_rows], send_sem=v_ss.at[head],
            recv_sem=v_rs.at[src], device_id={'cpi': base + dst_member}, device_id_type=MESH)

    def q_copy(head, dst_member, src):
        return pltpu.make_async_remote_copy(
            src_ref=q_out.at[head], dst_ref=q_in.at[src], send_sem=q_ss.at[head], recv_sem=q_rs.at[src],
            device_id={'cpi': base + dst_member}, device_id_type=MESH)

    def o_copy(block, head):
        return pltpu.make_async_remote_copy(
            src_ref=kv_out.at[block], dst_ref=o_in.at[head], send_sem=o_ss.at[block], recv_sem=o_rs.at[head],
            device_id={'cpi': base + block}, device_id_type=MESH)

    def halo(block):
        return pltpu.make_async_remote_copy(
            src_ref=kv_in.at[GROUP + block], dst_ref=kv_in.at[block], send_sem=h_ss.at[block], recv_sem=h_rs.at[block],
            device_id={'cpo': next_core, 'cpi': next_chip}, device_id_type=MESH)

    def send_class(copy, k):
        for step in range(4):
            y = (my_y + step) % 4
            head = 4 * class_chunk(k) + y

            def go(head=head):
                copy(head, member_of(head), me).start()

            if step == 0:
                pl.when(k > 0)(go)
            else:
                go()

    def kv_chunk(t, carry):
        c = (first + t) % 2
        k_all = project(0)
        for i in range(8):
            kv_out[8 * c + i, 0:TOK, :] = rope(k_all[:, HD * i:HD * i + HD]).astype(jnp.bfloat16)

        @pl.when(t == 0)
        def _():
            w_start(wk_hbm, 1 - first, 0)

        @pl.when(t == 1)
        def _():
            w_start(wq_hbm, class_chunk(0), 0)

        send_class(k_copy, t)
        send_class(k_copy, t + 2)

        v_all = project(1)
        for i in range(8):
            v_bf = v_all[:, HD * i:HD * i + HD].astype(jnp.bfloat16)
            kv_out[8 * c + i, TOK:TOK + HD, :] = v_bf[0:HD].T
            kv_out[8 * c + i, TOK + HD:TOK + 2 * HD, :] = v_bf[HD:TOK].T

        @pl.when(t == 0)
        def _():
            w_start(wv_hbm, 1 - first, 1)

        @pl.when(t == 1)
        def _():
            w_start(wq_hbm, class_chunk(1), 1)

        send_class(v_copy, t)
        send_class(v_copy, t + 2)
        return carry

    lax.fori_loop(0, 2, kv_chunk, 0)
    kv_in[BACK + me] = kv_out[my_head]

    def wait_kv(src):
        @pl.when(src != me)
        def _():
            k_copy(0, 0, src).wait_recv()
            v_copy(0, 0, src).wait_recv()

    def forward(parity):
        for i in range(4):
            y = 2 + i // 2
            src = 4 * y + (y + my_class + parity + 2 * (i % 2)) % 4
            wait_kv(src)
            halo(src - BACK).start()

    def q_store(slot, k):
        q_all = project(slot)
        j = class_chunk(k)
        for i in range(4):
            for g in range(2):
                lo = HD * (2 * i + g)
                q_out[4 * j + i, TOK * g:TOK * g + TOK, :] = rope(q_all[:, lo:lo + HD]).astype(jnp.bfloat16)

    def q_chunk(u, carry):
        for half in range(2):
            k = 2 * u + half
            q_store(half, k)

            @pl.when(u == 0)
            def _():
                w_start(wq_hbm, class_chunk(2 + half), half)

            send_class(q_copy, k)

            @pl.when(u == half)
            def _():
                forward(half)
        return carry

    lax.fori_loop(0, 2, q_chunk, 0)

    y_acc[...] = jnp.zeros_like(y_acc)
    n_wo = wo_buf.shape[0]

    def out_head(g):
        return 4 * class_chunk(g // 2) + 2 * (g % 2)

    def wo_copy(g):
        return pltpu.make_async_copy(wo_hbm.at[pl.ds(2 * out_head(g), 4)], wo_buf.at[g % n_wo], wo_sem.at[g % n_wo])

    for g in range(n_wo):
        wo_copy(g).start()

    q_in[me] = q_out[my_head]

    def kv_low(src, carry):
        wait_kv(src)
        return carry

    lax.fori_loop(0, BACK, kv_low, 0)

    def kv_drain(h, carry):
        @pl.when(h != my_head)
        def _():
            k_copy(h, 0, 0).wait_send()
            v_copy(h, 0, 0).wait_send()
        return carry

    lax.fori_loop(0, GROUP, kv_drain, 0)

    scale = HD ** -0.5 * math.log2(math.e)
    rows_k = lax.broadcasted_iota(jnp.int32, (TOK, 2 * TOK), 0)
    rows_q = lax.broadcasted_iota(jnp.int32, (TOK, 2 * TOK), 1) % TOK
    causal = rows_k <= rows_q
    is_first = (z == 0) & (core == 0)
    neg = jnp.float32(-jnp.inf)

    def biases(i):
        return [jnp.where(is_first & (i + j < BACK), neg, jnp.float32(0.0)) for j in range(BACK)]

    def scores(block, q):
        return lax.dot_general(kv_in[block, 0:TOK, :], q, (((1,), (1,)), ((), ())), preferred_element_type=jnp.float32)

    def v_of(block):
        return jnp.concatenate([kv_in[block, TOK:TOK + HD, :], kv_in[block, TOK + HD:TOK + 2 * HD, :]], axis=1)

    def score_tile(buf, i, q, j, bias, top):
        if j == 0:
            s = jnp.where(causal, scores(i + BACK, q), scores(i, q) + bias[0])
            buf[0] = s
            return jnp.max(s, axis=0, keepdims=True)
        s = scores(i + j, q)
        buf[j] = s
        return jnp.maximum(top, jnp.max(s, axis=0, keepdims=True) + bias[j])

    def pv_tile(buf, i, j, bias, top, total, acc):
        if j == 0:
            p = jnp.exp2(buf[0] * scale - top)
            zero = jnp.zeros_like(p)
            acc = jnp.dot(v_of(i + BACK), jnp.where(causal, p, zero).astype(jnp.bfloat16),
                          preferred_element_type=jnp.float32)
            acc += jnp.dot(v_of(i), jnp.where(causal, zero, p).astype(jnp.bfloat16),
                           preferred_element_type=jnp.float32)
            return jnp.sum(p, axis=0, keepdims=True), acc
        p = jnp.exp2(buf[j] * scale - (top - bias[j]))
        total = total + jnp.sum(p, axis=0, keepdims=True)
        return total, acc + jnp.dot(v_of(i + j), p.astype(jnp.bfloat16), preferred_element_type=jnp.float32)

    def stage(done, ahead):
        if ahead is not None:
            buf_n, i_n = ahead
            q = q_in[i_n]
            bias_n = biases(i_n)
        if done is not None:
            buf_d, i_d, top_d = done
            top_d = top_d * scale
            bias_d = biases(i_d)
        top_n = total = acc = None
        for j in range(BACK):
            if ahead is not None:
                top_n = score_tile(buf_n, i_n, q, j, bias_n, top_n)
            if done is not None:
                total, acc = pv_tile(buf_d, i_d, j, bias_d, top_d, total, acc)
        if done is not None:
            o = (acc / total).T
            kv_out[i_d] = o.astype(jnp.bfloat16)
        return top_n

    n_cols = d_model // 4

    def out_rows(head):
        return jnp.concatenate([o_in[head + k, TOK * g2:TOK * g2 + TOK] for k in range(2) for g2 in range(2)], axis=1)

    def out_ready(g):
        wo_copy(g).wait()
        head = out_head(g)
        for k in range(2):
            @pl.when(head + k != my_head)
            def _():
                o_copy(0, head + k).wait_recv()
        return head

    def out_step(g, carry):
        head = out_ready(g)
        o = out_rows(head)
        w = wo_buf[g % n_wo].reshape(4 * HD, d_model)
        for n in range(4):
            cols = slice(n_cols * n, n_cols * n + n_cols)
            y_acc[:, cols] += jnp.dot(o, w[:, cols], preferred_element_type=jnp.float32)

        @pl.when(g + n_wo < 8)
        def _():
            wo_copy(g + n_wo).start()
        return carry

    def out_last():
        head = out_ready(7)
        o = out_rows(head)
        w = wo_buf[7 % n_wo].reshape(4 * HD, d_model)
        copies = []
        for n in range(4):
            cols = slice(n_cols * n, n_cols * n + n_cols)
            y = y_acc[:, cols] + jnp.dot(o, w[:, cols], preferred_element_type=jnp.float32)
            x_v[:, cols] = y.astype(jnp.bfloat16)
            part = pl.ds(n_cols * n, n_cols)
            copies.append(pltpu.make_async_copy(x_v.at[:, part], y_hbm.at[:, part], y_sem.at[n]))
            copies[-1].start()
        return copies

    def attend_set(t, carry):
        blocks = []
        for n in range(4):
            y = (2 if n < 2 else 0) + (my_y + n) % 2
            blocks.append(4 * y + (y + my_class + 4 - t) % 4)
        bufs = (s_a, s_b, s_a, s_b)

        def wait_q(i):
            @pl.when(i != me)
            def _():
                q_copy(0, 0, i).wait_recv()

        def ship(i):
            @pl.when(i != me)
            def _():
                o_copy(i, my_head).start()

            @pl.when(i == me)
            def _():
                o_in[my_head] = kv_out[me]

        wait_q(blocks[0])
        top = stage(None, (bufs[0], blocks[0]))
        for n in range(4):
            if n == 1:
                @pl.when(t == 0)
                def _():
                    for b in range(BACK):
                        halo(b).wait_recv()
            if n < 3:
                wait_q(blocks[n + 1])
            top = stage((bufs[n], blocks[n], top), (bufs[n + 1], blocks[n + 1]) if n < 3 else None)
            ship(blocks[n])

        @pl.when(t > 0)
        def _():
            lax.fori_loop(t - 1, t, out_step, 0)
        return carry

    lax.fori_loop(0, 4, attend_set, 0)
    lax.fori_loop(3, 8, out_step, 0)
    y_copies = []
    for r in range(4):
        part = pl.ds(TOK // 4 * r, TOK // 4)
        x_v[part, :] = y_acc[part, :].astype(jnp.bfloat16)
        y_copies.append(pltpu.make_async_copy(x_v.at[part], y_hbm.at[part], y_sem.at[r]))
        y_copies[-1].start()

    for b in range(BACK):
        halo(b).wait_send()

    def drain(h, carry):
        @pl.when(h != my_head)
        def _():
            q_copy(h, 0, 0).wait_send()

        @pl.when(h != me)
        def _():
            o_copy(h, 0).wait_send()
        return carry

    lax.fori_loop(0, GROUP, drain, 0)
    for y_copy in y_copies:
        y_copy.wait()


def solution(mesh):
    n_inner = mesh.shape['cpi']

    def local_fn(hidden, w_q, w_k, w_v, w_o):
        tok, d_model = hidden.shape
        inv_freq = ROPE_BASE ** (-np.arange(HD // 2) * 2.0 / HD)
        freq = jnp.asarray(np.tile(np.concatenate([inv_freq, inv_freq])[None, :], (tok, 1)), jnp.float32)
        any_spec = pl.BlockSpec(memory_space=pl.ANY)
        bf = jnp.bfloat16
        dma = pltpu.SemaphoreType.DMA
        return pl.pallas_call(
            body,
            out_shape=jax.ShapeDtypeStruct((tok, d_model), bf),
            in_specs=[any_spec] * 6,
            out_specs=any_spec,
            scratch_shapes=[
                pltpu.VMEM((tok, d_model), bf),
                pltpu.VMEM((tok, HD), jnp.float32),
                pltpu.VMEM((tok, HD), jnp.float32),
                pltpu.VMEM((tok, HD), jnp.float32),
                pltpu.VMEM((d_model, 8, HD), bf),
                pltpu.VMEM((d_model, 8, HD), bf),
                pltpu.VMEM((GROUP, 2 * TOK, HD), bf),
                pltpu.VMEM((GROUP, 2 * TOK, HD), bf),
                pltpu.VMEM((GROUP + BACK, 2 * TOK, HD), bf),
                pltpu.VMEM((GROUP, 2 * TOK, HD), bf),
                pltpu.VMEM((BACK, TOK, 2 * TOK), jnp.float32),
                pltpu.VMEM((BACK, TOK, 2 * TOK), jnp.float32),
                pltpu.VMEM((GROUP, 2 * TOK, HD), bf),
                pltpu.VMEM((2, 4, HD, d_model), bf),
                pltpu.VMEM((tok, d_model), jnp.float32),
                dma((3,)), dma((2, 2)), dma((2,)), dma((4,)),
                dma((GROUP,)), dma((GROUP,)), dma((GROUP,)), dma((GROUP,)), dma((BACK,)), dma((BACK,)),
                dma((GROUP,)), dma((GROUP,)), dma((GROUP,)), dma((GROUP,)),
            ],
            compiler_params=pltpu.CompilerParams(collective_id=0, has_side_effects=True, vmem_limit_bytes=67043328),
        )(hidden, w_q, w_k, w_v, w_o, freq)

    return jax.shard_map(local_fn, mesh=mesh,
                         in_specs=(P(('dp', 'cpo', 'cpi'), None), P(), P(), P(), P()),
                         out_specs=P(('dp', 'cpo', 'cpi'), None), check_vma=False)
```
